32 devices in a mesh: dp: 4 (over y, x), frame: 8 (over z, core).
Axes of the slice: x: 2, y: 2, z: 4, core: 2. Of those that a mesh axis runs over, the one named last changes fastest.
Arguments:
- frames_in: bfloat16 [4, 8, 64, 1024], P('dp', 'frame'), may hold values from -6 to 6
- bottleneck: bfloat16 [4, 4, 1024], P('dp'), may hold values from -6 to 6
- spatial_entry: bfloat16 [1024, 1536], replicated, may hold values from -2 to 2
- spatial_exit: bfloat16 [1024, 512], replicated, may hold values from -0.25 to 0.25
- temporal_entry: bfloat16 [1024, 1536], replicated, may hold values from -2 to 2
- temporal_exit: bfloat16 [1024, 512], replicated, may hold values from -0.25 to 0.25
- output_grad: bfloat16 [4, 8, 64, 1024], P('dp', 'frame'), may hold values from -6 to 6
- joined_grad: bfloat16 [4, 4, 1024], P('dp'), may hold values from -6 to 6
Outputs:
- frames_delta: bfloat16 [4, 8, 64, 1024], P('dp', 'frame')
- bottleneck_delta: bfloat16 [4, 4, 1024], P('dp')
- spatialin_grad: bfloat16 [1024, 1536], P(('dp', 'frame'))
- spatialout_grad: bfloat16 [1024, 512], P(('dp', 'frame'))
- temporalin_grad: bfloat16 [1024, 1536], P(('dp', 'frame'))
- temporalout_grad: bfloat16 [1024, 512], P(('dp', 'frame'))
The draws below stay inside these ranges and needn't reach their ends.
All inputs are finite; a program needn't handle non-finite values.
Results may differ from the reference program's by a relative error of at most 0.024.
Values may be sent and summed in bfloat16 or wider, within the bound.
A program may use at most 64 MiB of HBM per device.

```python
import math
import jax
import jax.numpy as jnp
from jax import lax

D = 1024
HEAD = 64
HEADS = 8
BOT = 4
CLIPS = 4
FRAMES = 8
PATCHES = 64


def entry_draw(key):
    base_key = jax.random.fold_in(key, 0)
    drawn = jax.random.normal(base_key, (D, 3 * HEADS * HEAD), jnp.float32) / math.sqrt(D)
    return jnp.clip(drawn, -2.0, 2.0)


def draw_spatial_entry(key, part):
    return entry_draw(jax.random.fold_in(key, 17)).astype(jnp.bfloat16)


def draw_temporal_entry(key, part):
    return entry_draw(jax.random.fold_in(key, 29)).astype(jnp.bfloat16)


def strengthened(values, key, source, target, blocks, factor):
    owner, partner = [(jnp.arange(values.shape[dim]) // (values.shape[dim] // blocks)).reshape([-1 if axis == dim else 1 for axis in range(values.ndim)]) for dim in (source, target)]
    chosen = jax.random.permutation(key, blocks)[partner]
    strong = (owner == chosen) | (owner == (partner + blocks // 2) % blocks)
    return jnp.where(strong, factor * values, values)


def block_levels(stream_key, extent, cuts, least, largest):
    level = 1.0
    for dim, parts in cuts:
        draws = jax.random.uniform(jax.random.fold_in(jax.random.fold_in(stream_key, 6), dim), (parts,), jnp.float32, least / len(cuts), largest / len(cuts))
        level = level * jnp.repeat(jnp.exp(draws), extent[dim] // parts).reshape((-1,) + (1,) * (len(extent) - 1 - dim))
    return level


def scatter_about(own_key, dims, spread, limit, cuts=(), dtype=jnp.bfloat16):
    loudness = block_levels(own_key, dims, cuts, -0.22, 0.18) if cuts else 1.0
    array = jax.random.normal(own_key, dims, jnp.float32) * spread * loudness
    return jnp.minimum(jnp.maximum(array, -limit), limit).astype(dtype)


def noise_with(stream_key, shape, deviation, limit, cuts, heavy, dtype=jnp.bfloat16):
    values = deviation * jax.random.normal(stream_key, shape, jnp.float32)
    if cuts:
        values = values * block_levels(stream_key, shape, cuts, -0.22, 0.18)
    return jnp.clip(strengthened(values, jax.random.fold_in(stream_key, 3), *heavy), -limit, limit).astype(dtype)


def setup_inputs(seed: int = 0) -> dict:
    arg_keys = jax.random.split(jax.random.key(seed), 9)
    return {
        "frames_in": scatter_about(arg_keys[0], (CLIPS, FRAMES, PATCHES, D), 1.0, 6.0, ((0, 4), (1, 8))),
        "bottleneck": scatter_about(arg_keys[1], (CLIPS, BOT, D), 1.0, 6.0, ((0, 4),)),
        "spatial_entry": draw_spatial_entry(jax.random.fold_in(arg_keys[8], 71), 0),
        "spatial_exit": scatter_about(arg_keys[3], (D, HEADS * HEAD), (HEADS * HEAD) ** -0.5, 0.25),
        "temporal_entry": draw_temporal_entry(jax.random.fold_in(arg_keys[8], 71), 0),
        "temporal_exit": scatter_about(arg_keys[5], (D, HEADS * HEAD), (HEADS * HEAD) ** -0.5, 0.25),
        "output_grad": noise_with(arg_keys[6], (CLIPS, FRAMES, PATCHES, D), 1.0, 6.0, ((0, 4), (1, 8)), (1, 3, 8, 2.0)),
        "joined_grad": scatter_about(arg_keys[7], (CLIPS, BOT, D), 1.0, 6.0, ((0, 4),)),
    }


EPSILON = 1e-05

def product_form(form, left, right):
    left, right = lax.optimization_barrier((left, right))
    return jnp.einsum(form, left.astype(jnp.float32), right.astype(jnp.float32), preferred_element_type=jnp.float32)

def product_general(left, right, numbers):
    left, right = lax.optimization_barrier((left, right))
    return lax.dot_general(left.astype(jnp.float32), right.astype(jnp.float32), numbers, preferred_element_type=jnp.float32)

def normalize(inputs):
    widened = lax.optimization_barrier(inputs).astype(jnp.float32)
    centred = widened - lax.optimization_barrier(jnp.mean(widened, axis=-1, keepdims=True))
    inverse = lax.rsqrt(lax.optimization_barrier(jnp.mean(centred * centred, axis=-1, keepdims=True)) + EPSILON)
    return (centred * inverse, inverse)

def attend(inputs, entry_weight, head_count):
    normed, inverse = normalize(inputs)
    normed_low = normed.astype(jnp.bfloat16)
    mixture = product_general(normed_low, entry_weight, (((3,), (0,)), ((), ()))).astype(jnp.bfloat16)
    lead_count, seq_length, side_count = (inputs.shape[0], inputs.shape[1], inputs.shape[2])
    head_width = entry_weight.shape[1] // 3
    head_size = head_width // head_count
    pieces = mixture.reshape(lead_count, seq_length, side_count, 3, head_count, head_size)
    queries = pieces[:, :, :, 0]
    key_heads = pieces[:, :, :, 1]
    values = pieces[:, :, :, 2]
    factor = 1.0 / math.sqrt(head_size)
    scores = product_form('albhe,ambhe->abhlm', queries, key_heads) * factor
    scores = scores - lax.optimization_barrier(jnp.max(scores, axis=-1, keepdims=True))
    expon = jnp.exp(scores)
    softmax_weights = expon / lax.optimization_barrier(jnp.sum(expon, axis=-1, keepdims=True))
    softmax_low = softmax_weights.astype(jnp.bfloat16)
    attended = product_form('abhlm,ambhe->albhe', softmax_low, values).astype(jnp.bfloat16)
    attended = attended.reshape(lead_count, seq_length, side_count, head_width)
    return (normed, inverse, normed_low, queries, key_heads, values, softmax_weights, softmax_low, attended)

def project_out(inputs, attended, exit_weight):
    return lax.optimization_barrier(inputs).astype(jnp.float32) + product_general(attended, exit_weight, (((3,), (1,)), ((), ())))

def backward(cotangent, saved, entry_weight, exit_weight, head_count):
    normed, inverse, normed_low, queries, key_heads, values, softmax_weights, softmax_low, attended = saved
    lead_count, seq_length, side_count = (cotangent.shape[0], cotangent.shape[1], cotangent.shape[2])
    head_width = exit_weight.shape[1]
    head_size = head_width // head_count
    factor = 1.0 / math.sqrt(head_size)
    rows_dims = (((0, 1, 2), (0, 1, 2)), ((), ()))
    exit_grad = product_general(cotangent, attended, rows_dims)
    attended_grad = product_general(cotangent, exit_weight, (((3,), (0,)), ((), ()))).astype(jnp.bfloat16)
    attended_grad = attended_grad.reshape(lead_count, seq_length, side_count, head_count, head_size)
    softmax_grad = product_form('albhe,ambhe->abhlm', attended_grad, values)
    values_grad = product_form('abhlm,albhe->ambhe', softmax_low, attended_grad)
    centre = lax.optimization_barrier(jnp.sum(softmax_weights * softmax_grad, axis=-1, keepdims=True))
    scores_grad = (softmax_weights * (softmax_grad - centre) * factor).astype(jnp.bfloat16)
    queries_grad = product_form('abhlm,ambhe->albhe', scores_grad, key_heads)
    keys_grad = product_form('abhlm,albhe->ambhe', scores_grad, queries)
    mixture_grad = jnp.stack([queries_grad, keys_grad, values_grad], axis=3).astype(jnp.bfloat16)
    mixture_grad = mixture_grad.reshape(lead_count, seq_length, side_count, 3 * head_width)
    entry_grad = product_general(normed_low, mixture_grad, rows_dims)
    normed_grad = product_general(mixture_grad, entry_weight, (((3,), (1,)), ((), ())))
    inner_term = normed_grad - lax.optimization_barrier(jnp.mean(normed_grad, axis=-1, keepdims=True)) - normed * lax.optimization_barrier(jnp.mean(normed_grad * normed, axis=-1, keepdims=True))
    inputs_grad = lax.optimization_barrier(cotangent).astype(jnp.float32) + inverse * inner_term
    return (inputs_grad, entry_grad, exit_grad)

def reference(frames_in, bottleneck, spatial_entry, spatial_exit, temporal_entry, temporal_exit, output_grad, joined_grad):

    def per_clip(carry, items):
        frames, bottle, output_cot, joined_cot = items
        tokens_in = jnp.concatenate([frames, jnp.broadcast_to(bottle[None], (FRAMES, BOT, D))], axis=1)
        sequences = tokens_in[:, :, None, :]
        spatial_saved = attend(sequences, spatial_entry, HEADS)
        block_out = project_out(sequences, spatial_saved[8], spatial_exit)
        states = block_out[:, :PATCHES, 0, :].astype(jnp.bfloat16)[None]
        temporal_saved = attend(states, temporal_entry, HEADS)
        states_grad, temporal_in, temporal_out = backward(output_cot[None], temporal_saved, temporal_entry, temporal_exit, HEADS)
        state_grads = states_grad[0].astype(jnp.bfloat16)
        joined_rows = (lax.optimization_barrier(joined_cot).astype(jnp.float32) / FRAMES).astype(jnp.bfloat16)
        cotangent = jnp.concatenate([state_grads, jnp.broadcast_to(joined_rows[None], (FRAMES, BOT, D))], axis=1)[:, :, None, :]
        tokens_grad, spatial_in, spatial_out = backward(cotangent, spatial_saved, spatial_entry, spatial_exit, HEADS)
        frames_delta = tokens_grad[:, :PATCHES, 0, :].astype(jnp.bfloat16)
        bottleneck_delta = lax.optimization_barrier(jnp.sum(tokens_grad[:, PATCHES:, 0, :], axis=0)).astype(jnp.bfloat16)
        updated = (carry[0] + spatial_in, carry[1] + spatial_out, carry[2] + temporal_in, carry[3] + temporal_out)
        return (updated, (frames_delta, bottleneck_delta))
    start = (jnp.zeros((D, 3 * HEADS * HEAD), jnp.float32), jnp.zeros((D, HEADS * HEAD), jnp.float32), jnp.zeros((D, 3 * HEADS * HEAD), jnp.float32), jnp.zeros((D, HEADS * HEAD), jnp.float32))
    totals, stacked = lax.scan(per_clip, start, (frames_in, bottleneck, output_grad, joined_grad))
    grad_factor = 1.0 / math.sqrt(CLIPS * FRAMES * PATCHES)
    spatialin_grad = (totals[0] * grad_factor).astype(jnp.bfloat16)
    spatialout_grad = (totals[1] * grad_factor).astype(jnp.bfloat16)
    temporalin_grad = (totals[2] * grad_factor).astype(jnp.bfloat16)
    temporalout_grad = (totals[3] * grad_factor).astype(jnp.bfloat16)
    return (stacked[0], stacked[1], spatialin_grad, spatialout_grad, temporalin_grad, temporalout_grad)
```

```python
import functools
import math

import jax
import jax.numpy as jnp
from jax import lax
from jax.experimental import pallas as pl
from jax.experimental.pallas import tpu as pltpu
from jax.sharding import PartitionSpec as P

HEADS = 8
EPSILON = 1e-05
MESH = pl.DeviceIdType.MESH
F32 = jnp.float32
BF16 = jnp.bfloat16


def dot(left, right, left_dim=1, right_dim=0):
    return lax.dot_general(
        left, right, (((left_dim,), (right_dim,)), ((), ())), preferred_element_type=F32
    )


def normalize(widened):
    centred = widened - jnp.mean(widened, axis=-1, keepdims=True)
    inverse = lax.rsqrt(jnp.mean(centred * centred, axis=-1, keepdims=True) + EPSILON)
    return centred * inverse, inverse


def head_masks(width, dtype):
    lanes = lax.broadcasted_iota(jnp.int32, (1, width), 1)
    size = width // HEADS
    return [
        jnp.where((lanes >= h * size) & (lanes < (h + 1) * size), 1.0, 0.0).astype(dtype)
        for h in range(HEADS)
    ]


def stack_heads(rows):
    return jnp.concatenate([rows * m for m in head_masks(rows.shape[1], rows.dtype)], axis=0)


def merge_heads(stacked):
    count = stacked.shape[0] // HEADS
    masks = head_masks(stacked.shape[1], stacked.dtype)
    total = stacked[:count] * masks[0]
    for h in range(1, HEADS):
        total = total + stacked[h * count : (h + 1) * count] * masks[h]
    return total


def attend(normed_low, entry_ref, mask):
    mixture = dot(normed_low, entry_ref[...]).astype(BF16)
    width = mixture.shape[1] // 3
    queries, key_rows, values = (mixture[:, i * width : (i + 1) * width] for i in range(3))
    factor = 1.0 / math.sqrt(width // HEADS)
    query_stack = stack_heads(queries)
    scores = dot(query_stack, key_rows, 1, 1) * factor
    scores = jnp.where(mask, scores, -1e30)
    scores = scores - jnp.max(scores, axis=-1, keepdims=True)
    expon = jnp.where(mask, jnp.exp(scores), 0.0)
    weights = expon / jnp.sum(expon, axis=-1, keepdims=True)
    weights_low = weights.astype(BF16)
    attended = merge_heads(dot(weights_low, values)).astype(BF16)
    return attended, (query_stack, key_rows, values, weights, weights_low)


def backward_mixture(cotangent, exit_ref, saved):
    query_stack, key_rows, values, weights, weights_low = saved
    factor = 1.0 / math.sqrt(values.shape[1] // HEADS)
    attended_grad = dot(cotangent, exit_ref[...]).astype(BF16)
    grad_stack = stack_heads(attended_grad)
    softmax_grad = dot(grad_stack, values, 1, 1)
    values_grad = dot(weights_low, grad_stack, 0, 0)
    centre = jnp.sum(weights * softmax_grad, axis=-1, keepdims=True)
    scores_grad = (weights * (softmax_grad - centre) * factor).astype(BF16)
    queries_grad = merge_heads(dot(scores_grad, key_rows))
    keys_grad = dot(scores_grad, query_stack, 0, 0)
    return jnp.concatenate(
        [queries_grad.astype(BF16), keys_grad.astype(BF16), values_grad.astype(BF16)], axis=1
    )


def backward_inputs(mixture_grad, entry_ref, cotangent, normed, inverse):
    normed_grad = dot(mixture_grad, entry_ref[...], 1, 1)
    inner = (
        normed_grad
        - jnp.mean(normed_grad, axis=-1, keepdims=True)
        - normed * jnp.mean(normed_grad * normed, axis=-1, keepdims=True)
    )
    return cotangent + inverse * inner


def kernel(
    frame_groups,
    data_groups,
    grad_factor,
    frames_ref,
    bottle_ref,
    output_grad_ref,
    joined_ref,
    spatial_entry_hbm,
    spatial_exit_hbm,
    temporal_entry_hbm,
    temporal_exit_hbm,
    frames_delta_ref,
    bottle_delta_ref,
    spatialin_ref,
    spatialout_ref,
    temporalin_ref,
    temporalout_ref,
    se_ref,
    so_ref,
    te_ref,
    to_ref,
    tokens,
    cot_ref,
    s_normed,
    t_normed,
    og_recv,
    st_send,
    st_recv,
    sg_send,
    sg_recv,
    bot_send,
    bot_recv,
    s_nl_send,
    s_nl,
    s_att,
    s_c_send,
    s_c,
    s_mg,
    t_nl_send,
    t_nl,
    t_att,
    t_c_send,
    t_c,
    t_mg,
    s_rs_send,
    s_rs,
    t_rs_send,
    t_rs,
    load_sem,
    f_send_sem,
    f_recv_sem,
    d_send_sem,
    d_recv_sem,
):
    frame = lax.axis_index("frame")
    data = lax.axis_index("dp")
    patches, model = frames_ref.shape
    bottles = bottle_ref.shape[0]
    rows = tokens.shape[0]
    group = output_grad_ref.shape[1]

    loads = [
        pltpu.make_async_copy(src, dst, load_sem.at[i])
        for i, (src, dst) in enumerate(
            (
                (spatial_entry_hbm, se_ref),
                (spatial_exit_hbm, so_ref),
                (temporal_entry_hbm, te_ref),
                (temporal_exit_hbm, to_ref),
            )
        )
    ]
    for load in loads:
        load.start()

    barrier = pltpu.get_barrier_semaphore()
    for k in range(1, frame_groups):
        pl.semaphore_signal(
            barrier,
            inc=1,
            device_id={"frame": lax.rem(frame + k, frame_groups)},
            device_id_type=MESH,
        )
    for k in range(1, data_groups):
        pl.semaphore_signal(
            barrier, inc=1, device_id={"dp": lax.rem(data + k, data_groups)}, device_id_type=MESH
        )
    pl.semaphore_wait(barrier, frame_groups + data_groups - 2)

    pending = []

    def push(src_of, dst, axis, phase):
        count = frame_groups if axis == "frame" else data_groups
        me = frame if axis == "frame" else data
        send, recv = (f_send_sem, f_recv_sem) if axis == "frame" else (d_send_sem, d_recv_sem)
        copies = []
        for k in range(1, count):
            peer = lax.rem(me + k, count)
            copy = pltpu.make_async_remote_copy(
                src_ref=src_of(peer),
                dst_ref=dst.at[me],
                send_sem=send.at[phase, k],
                recv_sem=recv.at[phase, k],
                device_id={axis: peer},
                device_id_type=MESH,
            )
            copy.start()
            copies.append(copy)
        pending.extend(copies)
        return copies

    def arrive(copies):
        for copy in copies:
            copy.wait_recv()

    def exchange(send, dst, axis, phase):
        me = frame if axis == "frame" else data
        copies = push(lambda peer: send.at[peer], dst, axis, phase)
        dst[me] = send[me]
        return copies

    def spread(dst, axis, phase):
        me = frame if axis == "frame" else data
        return push(lambda peer: dst.at[me], dst, axis, phase)

    def put_columns(dst, value):
        width = value.shape[1] // data_groups
        for i in range(data_groups):
            dst[i] = value[:, i * width : (i + 1) * width]

    og_copies = exchange(output_grad_ref, og_recv, "frame", 0)

    tokens[:patches] = frames_ref[...].astype(F32)
    tokens[patches:] = jnp.zeros((rows - patches, model), F32)
    tokens[patches : patches + bottles] = bottle_ref[...].astype(F32)
    normed, s_inverse = normalize(tokens[...])
    s_normed[...] = normed
    s_low = normed.astype(BF16)
    loads[0].wait()
    columns = lax.broadcasted_iota(jnp.int32, (HEADS * rows, rows), 1)
    attended, s_saved = attend(s_low, se_ref, columns < patches + bottles)
    loads[1].wait()
    states = (tokens[:patches] + dot(attended[:patches], so_ref[...], 1, 1)).astype(BF16)
    st_send[...] = states.astype(F32).reshape(frame_groups, group, model).astype(BF16)
    st_copies = exchange(st_send, st_recv, "frame", 1)
    put_columns(s_nl_send, s_low)
    s_att[data] = attended
    s_early = exchange(s_nl_send, s_nl, "dp", 0) + spread(s_att, "dp", 1)

    arrive(st_copies)
    t_rows = frame_groups * group
    normed, t_inverse = normalize(st_recv[...].astype(F32).reshape(t_rows, model))
    t_normed[...] = normed
    t_low = normed.astype(BF16)
    loads[2].wait()
    shape = (HEADS * t_rows, t_rows)
    row_patch = lax.broadcasted_iota(jnp.int32, shape, 0) & (group - 1)
    column_patch = lax.broadcasted_iota(jnp.int32, shape, 1) & (group - 1)
    attended, t_saved = attend(t_low, te_ref, row_patch == column_patch)
    put_columns(t_nl_send, t_low)
    t_att[data] = attended
    t_copies = exchange(t_nl_send, t_nl, "dp", 2) + spread(t_att, "dp", 3)
    arrive(og_copies)
    t_cot = og_recv[...].astype(F32).reshape(t_rows, model)
    t_cot_low = t_cot.astype(BF16)
    loads[3].wait()
    mixture_grad = backward_mixture(t_cot_low, to_ref, t_saved)
    t_mg[data] = mixture_grad
    state_grads = backward_inputs(mixture_grad, te_ref, t_cot, t_normed[...], t_inverse)
    sg_send[...] = state_grads.reshape(frame_groups, group, model).astype(BF16)
    sg_copies = exchange(sg_send, sg_recv, "frame", 2)
    t_copies += spread(t_mg, "dp", 4)
    put_columns(t_c_send, t_cot_low)
    t_copies += exchange(t_c_send, t_c, "dp", 5)

    cot_ref[patches:] = jnp.zeros((rows - patches, model), F32)
    cot_ref[patches : patches + bottles] = (
        (joined_ref[...].astype(F32) / frame_groups).astype(BF16).astype(F32)
    )
    arrive(sg_copies)
    cot_ref[:patches] = sg_recv[...].astype(F32).reshape(patches, model)
    s_cot_low = cot_ref[...].astype(BF16)
    mixture_grad = backward_mixture(s_cot_low, so_ref, s_saved)
    s_mg[data] = mixture_grad
    s_copies = spread(s_mg, "dp", 6)
    put_columns(s_c_send, s_cot_low)
    s_copies += exchange(s_c_send, s_c, "dp", 7)
    tokens_grad = backward_inputs(mixture_grad, se_ref, cot_ref[...], s_normed[...], s_inverse)
    frames_delta_ref[...] = tokens_grad[:patches].astype(BF16)
    bot_send[...] = tokens_grad[patches : patches + bot_send.shape[0]]
    bot_recv[frame] = bot_send[...]
    bot_copies = push(lambda peer: bot_send, bot_recv, "frame", 3)

    def partial(low, mixture, cotangent, attended, send):
        count = low.shape[0] * low.shape[1]
        flat = lambda ref: ref[...].reshape(count, ref.shape[2])
        width = mixture.shape[2]
        entry = dot(flat(low), flat(mixture), 0, 0)
        send[:, :, :width] = entry.reshape(send.shape[0], send.shape[1], width).astype(BF16)
        leave = dot(flat(cotangent), flat(attended), 0, 0)
        send[:, :, width:] = leave.reshape(
            send.shape[0], send.shape[1], attended.shape[2]
        ).astype(BF16)

    def total(recv, entry_out, exit_out):
        summed = recv[0].astype(F32)
        for i in range(1, frame_groups):
            summed = summed + recv[i].astype(F32)
        summed = (summed * grad_factor).astype(BF16)
        width = entry_out.shape[1]
        entry_out[...] = summed[:, :width]
        exit_out[...] = summed[:, width:]

    arrive(t_copies)
    partial(t_nl, t_mg, t_c, t_att, t_rs_send)
    t_rs_copies = exchange(t_rs_send, t_rs, "frame", 4)
    arrive(s_early)
    arrive(s_copies)
    partial(s_nl, s_mg, s_c, s_att, s_rs_send)
    s_rs_copies = exchange(s_rs_send, s_rs, "frame", 5)

    arrive(bot_copies)
    bottle_total = bot_recv[0]
    for i in range(1, frame_groups):
        bottle_total = bottle_total + bot_recv[i]
    bottle_delta_ref[...] = bottle_total[:bottles].astype(BF16)
    arrive(t_rs_copies)
    total(t_rs, temporalin_ref, temporalout_ref)
    arrive(s_rs_copies)
    total(s_rs, spatialin_ref, spatialout_ref)
    for copy in pending:
        copy.wait_send()


def per_device(
    frames_in,
    bottleneck,
    spatial_entry,
    spatial_exit,
    temporal_entry,
    temporal_exit,
    output_grad,
    joined_grad,
):
    clip_count, frames_local, patches, model = frames_in.shape
    bottles = bottleneck.shape[1]
    frame_groups = lax.axis_size("frame")
    data_groups = lax.axis_size("dp")
    assert clip_count == 1 and frames_local == 1
    entry_width = spatial_entry.shape[1]
    exit_width = spatial_exit.shape[1]
    width = entry_width + exit_width
    group = patches // frame_groups
    assert group & (group - 1) == 0
    rows = -(-(patches + bottles) // 16) * 16
    t_rows = patches
    block = model // data_groups
    owned = block // frame_groups
    bottle_pad = -(-bottles // 8) * 8
    grad_factor = 1.0 / math.sqrt(patches * data_groups * frame_groups)

    def gather_set(count):
        return [
            pltpu.VMEM((data_groups, count, block), BF16),
            pltpu.VMEM((data_groups, count, block), BF16),
            pltpu.VMEM((data_groups, count, exit_width), BF16),
            pltpu.VMEM((data_groups, count, block), BF16),
            pltpu.VMEM((data_groups, count, block), BF16),
            pltpu.VMEM((data_groups, count, entry_width), BF16),
        ]

    moved = pltpu.VMEM((frame_groups, group, model), BF16)
    vmem = pl.BlockSpec(memory_space=pltpu.VMEM)
    hbm = pl.BlockSpec(memory_space=pl.ANY)
    outs = pl.pallas_call(
        functools.partial(kernel, frame_groups, data_groups, grad_factor),
        out_shape=(
            jax.ShapeDtypeStruct((patches, model), BF16),
            jax.ShapeDtypeStruct((bottles, model), BF16),
            jax.ShapeDtypeStruct((owned, entry_width), BF16),
            jax.ShapeDtypeStruct((owned, exit_width), BF16),
            jax.ShapeDtypeStruct((owned, entry_width), BF16),
            jax.ShapeDtypeStruct((owned, exit_width), BF16),
        ),
        in_specs=[vmem] * 4 + [hbm] * 4,
        out_specs=[vmem] * 6,
        scratch_shapes=[
            pltpu.VMEM(spatial_entry.shape, BF16),
            pltpu.VMEM(spatial_exit.shape, BF16),
            pltpu.VMEM(temporal_entry.shape, BF16),
            pltpu.VMEM(temporal_exit.shape, BF16),
            pltpu.VMEM((rows, model), F32),
            pltpu.VMEM((rows, model), F32),
            pltpu.VMEM((rows, model), F32),
            pltpu.VMEM((t_rows, model), F32),
            moved,
            moved,
            moved,
            moved,
            moved,
            pltpu.VMEM((bottle_pad, model), F32),
            pltpu.VMEM((frame_groups, bottle_pad, model), F32),
            *gather_set(rows),
            *gather_set(t_rows),
            *[pltpu.VMEM((frame_groups, owned, width), BF16)] * 4,
            pltpu.SemaphoreType.DMA((4,)),
            pltpu.SemaphoreType.DMA((6, frame_groups)),
            pltpu.SemaphoreType.DMA((6, frame_groups)),
            pltpu.SemaphoreType.DMA((8, data_groups)),
            pltpu.SemaphoreType.DMA((8, data_groups)),
        ],
        compiler_params=pltpu.CompilerParams(
            collective_id=0, has_side_effects=True, vmem_limit_bytes=60 * 1024 * 1024
        ),
    )(
        frames_in.reshape(patches, model),
        bottleneck.reshape(bottles, model),
        output_grad.reshape(frame_groups, group, model),
        joined_grad.reshape(bottles, model),
        spatial_entry,
        spatial_exit,
        temporal_entry,
        temporal_exit,
    )
    return (outs[0].reshape(frames_in.shape), outs[1].reshape(bottleneck.shape), *outs[2:])


def solution(mesh):
    return jax.shard_map(
        per_device,
        mesh=mesh,
        in_specs=(
            P("dp", "frame", None, None),
            P("dp", None, None),
            P(),
            P(),
            P(),
            P(),
            P("dp", "frame", None, None),
            P("dp", None, None),
        ),
        out_specs=(
            P("dp", "frame", None, None),
            P("dp", None, None),
            P(("dp", "frame"), None),
            P(("dp", "frame"), None),
            P(("dp", "frame"), None),
            P(("dp", "frame"), None),
        ),
        check_vma=False,
    )
```

```python
import functools
import math

import jax
import jax.numpy as jnp
from jax import lax
from jax.experimental import pallas as pl
from jax.experimental.pallas import tpu as pltpu
from jax.sharding import PartitionSpec as P

HEADS = 8
EPSILON = 1e-05
MESH = pl.DeviceIdType.MESH
F32 = jnp.float32
BF16 = jnp.bfloat16


def dot(left, right, left_dim=1, right_dim=0):
    return lax.dot_general(
        left, right, (((left_dim,), (right_dim,)), ((), ())), preferred_element_type=F32
    )


def normalize(widened):
    centred = widened - jnp.mean(widened, axis=-1, keepdims=True)
    inverse = lax.rsqrt(jnp.mean(centred * centred, axis=-1, keepdims=True) + EPSILON)
    return centred * inverse, inverse


def head_masks(width, dtype):
    lanes = lax.broadcasted_iota(jnp.int32, (1, width), 1)
    size = width // HEADS
    return [
        jnp.where((lanes >= h * size) & (lanes < (h + 1) * size), 1.0, 0.0).astype(dtype)
        for h in range(HEADS)
    ]


def stack_heads(rows):
    return jnp.concatenate([rows * m for m in head_masks(rows.shape[1], rows.dtype)], axis=0)


def merge_heads(stacked):
    count = stacked.shape[0] // HEADS
    masks = head_masks(stacked.shape[1], stacked.dtype)
    total = stacked[:count] * masks[0]
    for h in range(1, HEADS):
        total = total + stacked[h * count : (h + 1) * count] * masks[h]
    return total


def attend(normed_low, entry_ref, mask):
    mixture = dot(normed_low, entry_ref[...]).astype(BF16)
    width = mixture.shape[1] // 3
    queries, key_rows, values = (mixture[:, i * width : (i + 1) * width] for i in range(3))
    factor = 1.0 / math.sqrt(width // HEADS)
    query_stack = stack_heads(queries)
    scores = dot(query_stack, key_rows, 1, 1) * factor
    scores = jnp.where(mask, scores, -1e30)
    scores = scores - jnp.max(scores, axis=-1, keepdims=True)
    expon = jnp.where(mask, jnp.exp(scores), 0.0)
    weights = expon / jnp.sum(expon, axis=-1, keepdims=True)
    weights_low = weights.astype(BF16)
    attended = merge_heads(dot(weights_low, values)).astype(BF16)
    return attended, (query_stack, key_rows, values, weights, weights_low)


def backward_mixture(cotangent, exit_ref, saved, emit):
    query_stack, key_rows, values, weights, weights_low = saved
    factor = 1.0 / math.sqrt(values.shape[1] // HEADS)
    attended_grad = dot(cotangent, exit_ref[...]).astype(BF16)
    grad_stack = stack_heads(attended_grad)
    values_grad = dot(weights_low, grad_stack, 0, 0).astype(BF16)
    emit(2, values_grad)
    softmax_grad = dot(grad_stack, values, 1, 1)
    centre = jnp.sum(weights * softmax_grad, axis=-1, keepdims=True)
    scores_grad = (weights * (softmax_grad - centre) * factor).astype(BF16)
    keys_grad = dot(scores_grad, query_stack, 0, 0).astype(BF16)
    emit(1, keys_grad)
    queries_grad = merge_heads(dot(scores_grad, key_rows)).astype(BF16)
    emit(0, queries_grad)
    return jnp.concatenate([queries_grad, keys_grad, values_grad], axis=1)


def backward_inputs(mixture_grad, entry_ref, cotangent, normed, inverse):
    normed_grad = dot(mixture_grad, entry_ref[...], 1, 1)
    inner = (
        normed_grad
        - jnp.mean(normed_grad, axis=-1, keepdims=True)
        - normed * jnp.mean(normed_grad * normed, axis=-1, keepdims=True)
    )
    return cotangent + inverse * inner


def kernel(
    frame_groups,
    data_groups,
    grad_factor,
    frames_ref,
    bottle_ref,
    output_grad_ref,
    joined_ref,
    spatial_entry_hbm,
    spatial_exit_hbm,
    temporal_entry_hbm,
    temporal_exit_hbm,
    frames_delta_ref,
    bottle_delta_ref,
    spatialin_ref,
    spatialout_ref,
    temporalin_ref,
    temporalout_ref,
    se_ref,
    so_ref,
    te_ref,
    to_ref,
    tokens,
    cot_ref,
    s_normed,
    t_normed,
    og_recv,
    st_send,
    st_recv,
    sg_send,
    sg_recv,
    bot_send,
    bot_recv,
    s_nl_send,
    s_nl,
    s_att,
    s_c_send,
    s_c,
    s_mg,
    t_nl_send,
    t_nl,
    t_att,
    t_c_send,
    t_c,
    t_mg,
    part,
    pair_recv,
    row_send,
    row_recv,
    load_sem,
    f_send_sem,
    f_recv_sem,
    d_send_sem,
    d_recv_sem,
    pair_sem,
    r_send_sem,
    r_recv_sem,
):
    frame = lax.axis_index("frame")
    data = lax.axis_index("dp")
    patches, model = frames_ref.shape
    bottles = bottle_ref.shape[0]
    rows = tokens.shape[0]
    group = output_grad_ref.shape[1]

    loads = [
        pltpu.make_async_copy(src, dst, load_sem.at[i])
        for i, (src, dst) in enumerate(
            (
                (spatial_entry_hbm, se_ref),
                (spatial_exit_hbm, so_ref),
                (temporal_entry_hbm, te_ref),
                (temporal_exit_hbm, to_ref),
            )
        )
    ]
    for load in loads:
        load.start()

    barrier = pltpu.get_barrier_semaphore()
    for k in range(1, frame_groups):
        pl.semaphore_signal(
            barrier,
            inc=1,
            device_id={"frame": lax.rem(frame + k, frame_groups)},
            device_id_type=MESH,
        )
    for k in range(1, data_groups):
        pl.semaphore_signal(
            barrier, inc=1, device_id={"dp": lax.rem(data + k, data_groups)}, device_id_type=MESH
        )
    pl.semaphore_wait(barrier, frame_groups + data_groups - 2)

    pending = []

    def push(src_of, dst, axis, phase):
        count = frame_groups if axis == "frame" else data_groups
        me = frame if axis == "frame" else data
        send, recv = (f_send_sem, f_recv_sem) if axis == "frame" else (d_send_sem, d_recv_sem)
        copies = []
        for k in range(1, count):
            peer = lax.rem(me + k, count)
            copy = pltpu.make_async_remote_copy(
                src_ref=src_of(peer),
                dst_ref=dst.at[me],
                send_sem=send.at[phase, k],
                recv_sem=recv.at[phase, k],
                device_id={axis: peer},
                device_id_type=MESH,
            )
            copy.start()
            copies.append(copy)
        pending.extend(copies)
        return copies

    def arrive(copies):
        for copy in copies:
            copy.wait_recv()

    def exchange(send, dst, axis, phase):
        me = frame if axis == "frame" else data
        copies = push(lambda peer: send.at[peer], dst, axis, phase)
        dst[me] = send[me]
        return copies

    def spread(dst, axis, phase):
        me = frame if axis == "frame" else data
        return push(lambda peer: dst.at[me], dst, axis, phase)

    def put_columns(dst, value):
        width = value.shape[1] // data_groups
        for i in range(data_groups):
            dst[i] = value[:, i * width : (i + 1) * width]

    og_copies = exchange(output_grad_ref, og_recv, "frame", 0)

    tokens[:patches] = frames_ref[...].astype(F32)
    tokens[patches:] = jnp.zeros((rows - patches, model), F32)
    tokens[patches : patches + bottles] = bottle_ref[...].astype(F32)
    normed, s_inverse = normalize(tokens[...])
    s_normed[...] = normed
    s_low = normed.astype(BF16)
    loads[0].wait()
    columns = lax.broadcasted_iota(jnp.int32, (HEADS * rows, rows), 1)
    attended, s_saved = attend(s_low, se_ref, columns < patches + bottles)
    loads[1].wait()
    states = (tokens[:patches] + dot(attended[:patches], so_ref[...], 1, 1)).astype(BF16)
    st_send[...] = states.astype(F32).reshape(frame_groups, group, model).astype(BF16)
    st_copies = exchange(st_send, st_recv, "frame", 1)
    put_columns(s_nl_send, s_low)
    s_att[data] = attended
    s_early = exchange(s_nl_send, s_nl, "dp", 0) + spread(s_att, "dp", 1)

    arrive(st_copies)
    t_rows = frame_groups * group
    normed, t_inverse = normalize(st_recv[...].astype(F32).reshape(t_rows, model))
    t_normed[...] = normed
    t_low = normed.astype(BF16)
    loads[2].wait()
    shape = (HEADS * t_rows, t_rows)
    row_patch = lax.broadcasted_iota(jnp.int32, shape, 0) & (group - 1)
    column_patch = lax.broadcasted_iota(jnp.int32, shape, 1) & (group - 1)
    attended, t_saved = attend(t_low, te_ref, row_patch == column_patch)
    put_columns(t_nl_send, t_low)
    t_att[data] = attended
    t_copies = exchange(t_nl_send, t_nl, "dp", 2) + spread(t_att, "dp", 3)
    arrive(og_copies)
    t_cot = og_recv[...].astype(F32).reshape(t_rows, model)
    t_cot_low = t_cot.astype(BF16)
    loads[3].wait()

    def keep(i, value):
        t_mg[i, data] = value

    mixture_grad = backward_mixture(t_cot_low, to_ref, t_saved, keep)
    state_grads = backward_inputs(mixture_grad, te_ref, t_cot, t_normed[...], t_inverse)
    sg_send[...] = state_grads.reshape(frame_groups, group, model).astype(BF16)
    sg_copies = exchange(sg_send, sg_recv, "frame", 2)
    put_columns(t_c_send, t_cot_low)
    t_copies += exchange(t_c_send, t_c, "dp", 4)
    t_copies += [c for i in (2, 1, 0) for c in spread(t_mg.at[i], "dp", 5 + i)]

    cot_ref[patches:] = jnp.zeros((rows - patches, model), F32)
    cot_ref[patches : patches + bottles] = (
        (joined_ref[...].astype(F32) / frame_groups).astype(BF16).astype(F32)
    )
    arrive(sg_copies)
    cot_ref[:patches] = sg_recv[...].astype(F32).reshape(patches, model)
    s_cot_low = cot_ref[...].astype(BF16)
    put_columns(s_c_send, s_cot_low)
    s_early += exchange(s_c_send, s_c, "dp", 8)
    s_copies = {}

    def keep_and_send(i, value):
        s_mg[i, data] = value
        s_copies[i] = spread(s_mg.at[i], "dp", 9 + i)

    mixture_grad = backward_mixture(s_cot_low, so_ref, s_saved, keep_and_send)
    tokens_grad = backward_inputs(mixture_grad, se_ref, cot_ref[...], s_normed[...], s_inverse)
    frames_delta_ref[...] = tokens_grad[:patches].astype(BF16)
    bot_send[...] = tokens_grad[patches : patches + bottles]
    bot_recv[frame] = bot_send[...]
    bot_copies = push(lambda peer: bot_send, bot_recv, "frame", 3)

    side = lax.rem(frame, 2)
    chip = frame // 2
    chips = frame_groups // 2
    owned = part.shape[3]

    def partial(slot, left, right):
        count = left.shape[0] * left.shape[1]
        product = dot(
            left[...].reshape(count, left.shape[2]), right[...].reshape(count, right.shape[2]), 0, 0
        ).astype(BF16)
        for i in range(frame_groups):
            part[slot, i % 2, i // 2] = product[i * owned : (i + 1) * owned]
        copy = pltpu.make_async_remote_copy(
            src_ref=part.at[slot, 1 - side],
            dst_ref=pair_recv.at[slot],
            send_sem=pair_sem.at[0, slot],
            recv_sem=pair_sem.at[1, slot],
            device_id={"frame": chip * 2 + 1 - side},
            device_id_type=MESH,
        )
        copy.start()
        pending.append(copy)
        return copy

    def pass_on(slot, pair_copy):
        pair_copy.wait_recv()
        row_send[slot] = (part[slot, side].astype(F32) + pair_recv[slot].astype(F32)).astype(BF16)
        row_recv[slot, chip] = row_send[slot, chip]
        copies = []
        for k in range(1, chips):
            peer = lax.rem(chip + k, chips)
            copy = pltpu.make_async_remote_copy(
                src_ref=row_send.at[slot, peer],
                dst_ref=row_recv.at[slot, chip],
                send_sem=r_send_sem.at[slot, k],
                recv_sem=r_recv_sem.at[slot, k],
                device_id={"frame": peer * 2 + side},
                device_id_type=MESH,
            )
            copy.start()
            copies.append(copy)
        pending.extend(copies)
        return copies

    width = s_att.shape[2]
    work = [
        (t_copies, t_c, t_att, temporalout_ref, 0),
        ([], t_nl, t_mg.at[2], temporalin_ref, 2 * width),
        ([], t_nl, t_mg.at[1], temporalin_ref, width),
        ([], t_nl, t_mg.at[0], temporalin_ref, 0),
        (s_early, s_c, s_att, spatialout_ref, 0),
        (s_copies[2], s_nl, s_mg.at[2], spatialin_ref, 2 * width),
        (s_copies[1], s_nl, s_mg.at[1], spatialin_ref, width),
        (s_copies[0], s_nl, s_mg.at[0], spatialin_ref, 0),
    ]
    pair_copies, row_copies = [], []
    for slot, (needed, left, right, _, _) in enumerate(work):
        arrive(needed)
        pair_copies.append(partial(slot, left, right))
        if slot:
            row_copies.append(pass_on(slot - 1, pair_copies[slot - 1]))
    row_copies.append(pass_on(len(work) - 1, pair_copies[-1]))

    arrive(bot_copies)
    bottle_total = bot_recv[0]
    for i in range(1, frame_groups):
        bottle_total = bottle_total + bot_recv[i]
    bottle_delta_ref[...] = bottle_total.astype(BF16)
    for slot, (_, _, _, out, start) in enumerate(work):
        arrive(row_copies[slot])
        summed = row_recv[slot, 0].astype(F32)
        for i in range(1, chips):
            summed = summed + row_recv[slot, i].astype(F32)
        out[:, start : start + width] = (summed * grad_factor).astype(BF16)
    for copy in pending:
        copy.wait_send()


def hand_over(*refs):
    count = len(refs) // 2
    for source, target in zip(refs[:count], refs[count:]):
        target[...] = source[...]


def per_device(
    frames_in,
    bottleneck,
    spatial_entry,
    spatial_exit,
    temporal_entry,
    temporal_exit,
    output_grad,
    joined_grad,
):
    clip_count, frames_local, patches, model = frames_in.shape
    bottles = bottleneck.shape[1]
    frame_groups = lax.axis_size("frame")
    data_groups = lax.axis_size("dp")
    assert clip_count == 1 and frames_local == 1
    entry_width = spatial_entry.shape[1]
    exit_width = spatial_exit.shape[1]
    group = patches // frame_groups
    assert group & (group - 1) == 0 and frame_groups % 2 == 0
    assert entry_width == 3 * exit_width
    chips = frame_groups // 2
    rows = -(-(patches + bottles) // 16) * 16
    t_rows = patches
    block = model // data_groups
    owned = block // frame_groups
    grad_factor = 1.0 / math.sqrt(patches * data_groups * frame_groups)

    def gather_set(count):
        return [
            pltpu.VMEM((data_groups, count, block), BF16),
            pltpu.VMEM((data_groups, count, block), BF16),
            pltpu.VMEM((data_groups, count, exit_width), BF16),
            pltpu.VMEM((data_groups, count, block), BF16),
            pltpu.VMEM((data_groups, count, block), BF16),
            pltpu.VMEM((3, data_groups, count, exit_width), BF16),
        ]

    moved = pltpu.VMEM((frame_groups, group, model), BF16)
    vmem = pl.BlockSpec(memory_space=pltpu.VMEM)
    hbm = pl.BlockSpec(memory_space=pl.ANY)
    outs = pl.pallas_call(
        functools.partial(kernel, frame_groups, data_groups, grad_factor),
        out_shape=(
            jax.ShapeDtypeStruct((patches, model), BF16),
            jax.ShapeDtypeStruct((bottles, model), BF16),
            jax.ShapeDtypeStruct((owned, entry_width), BF16),
            jax.ShapeDtypeStruct((owned, exit_width), BF16),
            jax.ShapeDtypeStruct((owned, entry_width), BF16),
            jax.ShapeDtypeStruct((owned, exit_width), BF16),
        ),
        in_specs=[vmem] * 4 + [hbm] * 4,
        out_specs=[vmem] * 6,
        scratch_shapes=[
            pltpu.VMEM(spatial_entry.shape, BF16),
            pltpu.VMEM(spatial_exit.shape, BF16),
            pltpu.VMEM(temporal_entry.shape, BF16),
            pltpu.VMEM(temporal_exit.shape, BF16),
            pltpu.VMEM((rows, model), F32),
            pltpu.VMEM((rows, model), F32),
            pltpu.VMEM((rows, model), F32),
            pltpu.VMEM((t_rows, model), F32),
            moved,
            moved,
            moved,
            moved,
            moved,
            pltpu.VMEM((bottles, model), F32),
            pltpu.VMEM((frame_groups, bottles, model), F32),
            *gather_set(rows),
            *gather_set(t_rows),
            pltpu.VMEM((8, 2, chips, owned, exit_width), BF16),
            *[pltpu.VMEM((8, chips, owned, exit_width), BF16)] * 3,
            pltpu.SemaphoreType.DMA((4,)),
            pltpu.SemaphoreType.DMA((6, frame_groups)),
            pltpu.SemaphoreType.DMA((6, frame_groups)),
            pltpu.SemaphoreType.DMA((12, data_groups)),
            pltpu.SemaphoreType.DMA((12, data_groups)),
            pltpu.SemaphoreType.DMA((2, 8)),
            pltpu.SemaphoreType.DMA((8, chips)),
            pltpu.SemaphoreType.DMA((8, chips)),
        ],
        compiler_params=pltpu.CompilerParams(
            collective_id=0, has_side_effects=True, vmem_limit_bytes=61 * 1024 * 1024
        ),
    )(
        frames_in.reshape(patches, model),
        bottleneck.reshape(bottles, model),
        output_grad.reshape(frame_groups, group, model),
        joined_grad.reshape(bottles, model),
        spatial_entry,
        spatial_exit,
        temporal_entry,
        temporal_exit,
    )
    outs = pl.pallas_call(
        hand_over,
        out_shape=[jax.ShapeDtypeStruct(out.shape, out.dtype) for out in outs],
        in_specs=[vmem] * len(outs),
        out_specs=[vmem] * len(outs),
        compiler_params=pltpu.CompilerParams(vmem_limit_bytes=61 * 1024 * 1024),
    )(*outs)
    return (outs[0].reshape(frames_in.shape), outs[1].reshape(bottleneck.shape), *outs[2:])


def solution(mesh):
    return jax.shard_map(
        per_device,
        mesh=mesh,
        in_specs=(
            P("dp", "frame", None, None),
            P("dp", None, None),
            P(),
            P(),
            P(),
            P(),
            P("dp", "frame", None, None),
            P("dp", None, None),
        ),
        out_specs=(
            P("dp", "frame", None, None),
            P("dp", None, None),
            P(("dp", "frame"), None),
            P(("dp", "frame"), None),
            P(("dp", "frame"), None),
            P(("dp", "frame"), None),
        ),
        check_vma=False,
    )
```

```python
import functools
import math

import jax
import jax.numpy as jnp
from jax import lax
from jax.experimental import pallas as pl
from jax.experimental.pallas import tpu as pltpu
from jax.sharding import PartitionSpec as P

HEADS = 8
EPSILON = 1e-05
MESH = pl.DeviceIdType.MESH
F32 = jnp.float32
BF16 = jnp.bfloat16


def dot(left, right, left_dim=1, right_dim=0):
    return lax.dot_general(
        left, right, (((left_dim,), (right_dim,)), ((), ())), preferred_element_type=F32
    )


def normalize(widened):
    centred = widened - jnp.mean(widened, axis=-1, keepdims=True)
    inverse = lax.rsqrt(jnp.mean(centred * centred, axis=-1, keepdims=True) + EPSILON)
    return centred * inverse, inverse


def head_masks(width, dtype):
    lanes = lax.broadcasted_iota(jnp.int32, (1, width), 1)
    size = width // HEADS
    return [
        jnp.where((lanes >= h * size) & (lanes < (h + 1) * size), 1.0, 0.0).astype(dtype)
        for h in range(HEADS)
    ]


def stack_heads(rows):
    return jnp.concatenate([rows * m for m in head_masks(rows.shape[1], rows.dtype)], axis=0)


def merge_heads(stacked):
    count = stacked.shape[0] // HEADS
    masks = head_masks(stacked.shape[1], stacked.dtype)
    total = stacked[:count] * masks[0]
    for h in range(1, HEADS):
        total = total + stacked[h * count : (h + 1) * count] * masks[h]
    return total


def attend(normed_low, entry_ref, mask):
    mixture = dot(normed_low, entry_ref[...]).astype(BF16)
    width = mixture.shape[1] // 3
    queries, key_rows, values = (mixture[:, i * width : (i + 1) * width] for i in range(3))
    factor = 1.0 / math.sqrt(width // HEADS)
    query_stack = stack_heads(queries)
    scores = dot(query_stack, key_rows, 1, 1) * factor
    scores = jnp.where(mask, scores, -1e30)
    scores = scores - jnp.max(scores, axis=-1, keepdims=True)
    expon = jnp.where(mask, jnp.exp(scores), 0.0)
    weights = expon / jnp.sum(expon, axis=-1, keepdims=True)
    weights_low = weights.astype(BF16)
    attended = merge_heads(dot(weights_low, values)).astype(BF16)
    return attended, (query_stack, key_rows, values, weights, weights_low)


def backward_mixture(cotangent, exit_ref, saved, emit):
    query_stack, key_rows, values, weights, weights_low = saved
    factor = 1.0 / math.sqrt(values.shape[1] // HEADS)
    attended_grad = dot(cotangent, exit_ref[...]).astype(BF16)
    grad_stack = stack_heads(attended_grad)
    values_grad = dot(weights_low, grad_stack, 0, 0).astype(BF16)
    emit(2, values_grad)
    softmax_grad = dot(grad_stack, values, 1, 1)
    centre = jnp.sum(weights * softmax_grad, axis=-1, keepdims=True)
    scores_grad = (weights * (softmax_grad - centre) * factor).astype(BF16)
    keys_grad = dot(scores_grad, query_stack, 0, 0).astype(BF16)
    emit(1, keys_grad)
    queries_grad = merge_heads(dot(scores_grad, key_rows)).astype(BF16)
    emit(0, queries_grad)
    return jnp.concatenate([queries_grad, keys_grad, values_grad], axis=1)


def backward_inputs(mixture_grad, entry_ref, cotangent, normed, inverse):
    normed_grad = dot(mixture_grad, entry_ref[...], 1, 1)
    inner = (
        normed_grad
        - jnp.mean(normed_grad, axis=-1, keepdims=True)
        - normed * jnp.mean(normed_grad * normed, axis=-1, keepdims=True)
    )
    return cotangent + inverse * inner


def kernel(
    frame_groups,
    data_groups,
    grad_factor,
    frames_ref,
    bottle_ref,
    output_grad_ref,
    joined_ref,
    spatial_entry_hbm,
    spatial_exit_hbm,
    temporal_entry_hbm,
    temporal_exit_hbm,
    frames_delta_ref,
    bottle_delta_ref,
    spatialin_ref,
    spatialout_ref,
    temporalin_ref,
    temporalout_ref,
    se_ref,
    so_ref,
    te_ref,
    to_ref,
    tokens,
    cot_ref,
    s_normed,
    t_normed,
    og_recv,
    st_send,
    st_recv,
    sg_send,
    sg_recv,
    bot_send,
    bot_pair,
    bot_sum,
    bot_recv,
    s_nl_send,
    s_nl,
    s_att,
    s_c_send,
    s_c,
    s_mg,
    t_nl_send,
    t_nl,
    t_att,
    t_c_send,
    t_c,
    t_mg,
    part,
    pair_recv,
    row_send,
    row_recv,
    load_sem,
    f_send_sem,
    f_recv_sem,
    d_send_sem,
    d_recv_sem,
    pair_sem,
    r_send_sem,
    r_recv_sem,
):
    frame = lax.axis_index("frame")
    data = lax.axis_index("dp")
    patches, model = frames_ref.shape
    bottles = bottle_ref.shape[0]
    rows = tokens.shape[0]
    group = output_grad_ref.shape[1]

    loads = [
        pltpu.make_async_copy(src, dst, load_sem.at[i])
        for i, (src, dst) in enumerate(
            (
                (spatial_entry_hbm, se_ref),
                (spatial_exit_hbm, so_ref),
                (temporal_entry_hbm, te_ref),
                (temporal_exit_hbm, to_ref),
            )
        )
    ]
    loads[0].start()
    loads[1].start()

    barrier = pltpu.get_barrier_semaphore()
    for k in range(1, frame_groups):
        pl.semaphore_signal(
            barrier,
            inc=1,
            device_id={"frame": lax.rem(frame + k, frame_groups)},
            device_id_type=MESH,
        )
    for k in range(1, data_groups):
        pl.semaphore_signal(
            barrier, inc=1, device_id={"dp": lax.rem(data + k, data_groups)}, device_id_type=MESH
        )
    pl.semaphore_wait(barrier, frame_groups + data_groups - 2)

    pending = []

    def push(src_of, dst, axis, phase):
        count = frame_groups if axis == "frame" else data_groups
        me = frame if axis == "frame" else data
        send, recv = (f_send_sem, f_recv_sem) if axis == "frame" else (d_send_sem, d_recv_sem)
        copies = []
        for k in range(1, count):
            peer = lax.rem(me + k, count)
            copy = pltpu.make_async_remote_copy(
                src_ref=src_of(peer),
                dst_ref=dst.at[me],
                send_sem=send.at[phase, k],
                recv_sem=recv.at[phase, k],
                device_id={axis: peer},
                device_id_type=MESH,
            )
            copy.start()
            copies.append(copy)
        pending.extend(copies)
        return copies

    def arrive(copies):
        for copy in copies:
            copy.wait_recv()

    def exchange(send, dst, axis, phase):
        me = frame if axis == "frame" else data
        copies = push(lambda peer: send.at[peer], dst, axis, phase)
        dst[me] = send[me]
        return copies

    def spread(dst, axis, phase):
        me = frame if axis == "frame" else data
        return push(lambda peer: dst.at[me], dst, axis, phase)

    def put_columns(dst, value):
        width = value.shape[1] // data_groups
        for i in range(data_groups):
            dst[i] = value[:, i * width : (i + 1) * width]

    og_copies = exchange(output_grad_ref, og_recv, "frame", 0)

    tokens[:patches] = frames_ref[...].astype(F32)
    tokens[patches:] = jnp.zeros((rows - patches, model), F32)
    tokens[patches : patches + bottles] = bottle_ref[...].astype(F32)
    normed, s_inverse = normalize(tokens[...])
    s_normed[...] = normed
    s_low = normed.astype(BF16)
    loads[0].wait()
    loads[2].start()
    loads[3].start()
    columns = lax.broadcasted_iota(jnp.int32, (HEADS * rows, rows), 1)
    attended, s_saved = attend(s_low, se_ref, columns < patches + bottles)
    loads[1].wait()
    states = (tokens[:patches] + dot(attended[:patches], so_ref[...], 1, 1)).astype(BF16)
    st_send[...] = states.astype(F32).reshape(frame_groups, group, model).astype(BF16)
    st_copies = exchange(st_send, st_recv, "frame", 1)
    put_columns(s_nl_send, s_low)
    s_att[data] = attended
    s_early = exchange(s_nl_send, s_nl, "dp", 0) + spread(s_att, "dp", 1)

    t_rows = frame_groups * group
    arrive(og_copies)
    t_cot = og_recv[...].astype(F32).reshape(t_rows, model)
    t_cot_low = t_cot.astype(BF16)
    put_columns(t_c_send, t_cot_low)
    t_early = exchange(t_c_send, t_c, "dp", 4)
    arrive(st_copies)
    normed, t_inverse = normalize(st_recv[...].astype(F32).reshape(t_rows, model))
    t_normed[...] = normed
    t_low = normed.astype(BF16)
    loads[2].wait()
    shape = (HEADS * t_rows, t_rows)
    row_patch = lax.broadcasted_iota(jnp.int32, shape, 0) & (group - 1)
    column_patch = lax.broadcasted_iota(jnp.int32, shape, 1) & (group - 1)
    attended, t_saved = attend(t_low, te_ref, row_patch == column_patch)
    t_att[data] = attended
    t_early += spread(t_att, "dp", 3)
    put_columns(t_nl_send, t_low)
    t_nl_copies = exchange(t_nl_send, t_nl, "dp", 2)
    loads[3].wait()
    t_copies = {}

    def keep_temporal(i, value):
        t_mg[i, data] = value
        t_copies[i] = spread(t_mg.at[i], "dp", 5 + i)

    mixture_grad = backward_mixture(t_cot_low, to_ref, t_saved, keep_temporal)
    state_grads = backward_inputs(mixture_grad, te_ref, t_cot, t_normed[...], t_inverse)
    sg_send[...] = state_grads.reshape(frame_groups, group, model).astype(BF16)
    sg_copies = exchange(sg_send, sg_recv, "frame", 2)

    side = lax.rem(frame, 2)
    chip = frame // 2
    chips = frame_groups // 2
    owned = part.shape[3]

    def to_partner(src, dst, slot):
        copy = pltpu.make_async_remote_copy(
            src_ref=src,
            dst_ref=dst,
            send_sem=pair_sem.at[0, slot],
            recv_sem=pair_sem.at[1, slot],
            device_id={"frame": chip * 2 + 1 - side},
            device_id_type=MESH,
        )
        copy.start()
        pending.append(copy)
        return copy

    def to_chips(src_of, dst, slot):
        copies = []
        for k in range(1, chips):
            peer = lax.rem(chip + k, chips)
            copy = pltpu.make_async_remote_copy(
                src_ref=src_of(peer),
                dst_ref=dst,
                send_sem=r_send_sem.at[slot, k],
                recv_sem=r_recv_sem.at[slot, k],
                device_id={"frame": peer * 2 + side},
                device_id_type=MESH,
            )
            copy.start()
            copies.append(copy)
        pending.extend(copies)
        return copies

    def partial(slot, left, right):
        count = left.shape[0] * left.shape[1]
        product = dot(
            left[...].reshape(count, left.shape[2]), right[...].reshape(count, right.shape[2]), 0, 0
        ).astype(BF16)
        for i in range(frame_groups):
            part[slot, i % 2, i // 2] = product[i * owned : (i + 1) * owned]
        return to_partner(part.at[slot, 1 - side], pair_recv.at[slot], slot)

    def pass_on(slot, pair_copy):
        pair_copy.wait_recv()
        row_send[slot] = (part[slot, side].astype(F32) + pair_recv[slot].astype(F32)).astype(BF16)
        row_recv[slot, chip] = row_send[slot, chip]
        return to_chips(
            lambda peer: row_send.at[slot, peer], row_recv.at[slot, chip], slot
        )

    arrive(t_early)
    exit_pair = partial(0, t_c, t_att)

    cot_ref[patches:] = jnp.zeros((rows - patches, model), F32)
    cot_ref[patches : patches + bottles] = (
        (joined_ref[...].astype(F32) / frame_groups).astype(BF16).astype(F32)
    )
    exit_rows = pass_on(0, exit_pair)
    arrive(sg_copies)
    cot_ref[:patches] = sg_recv[...].astype(F32).reshape(patches, model)
    s_cot_low = cot_ref[...].astype(BF16)
    put_columns(s_c_send, s_cot_low)
    s_early += exchange(s_c_send, s_c, "dp", 8)
    s_copies = {}

    def keep_and_send(i, value):
        s_mg[i, data] = value
        s_copies[i] = spread(s_mg.at[i], "dp", 9 + i)

    mixture_grad = backward_mixture(s_cot_low, so_ref, s_saved, keep_and_send)
    tokens_grad = backward_inputs(mixture_grad, se_ref, cot_ref[...], s_normed[...], s_inverse)
    frames_delta_ref[...] = tokens_grad[:patches].astype(BF16)
    bot_send[...] = tokens_grad[patches : patches + bottles]
    last_slot = part.shape[0]
    bot_pair_copy = to_partner(bot_send, bot_pair, last_slot)

    width = s_att.shape[2]
    work = [
        ([], t_c, t_att, temporalout_ref, 0),
        (t_nl_copies + t_copies[2], t_nl, t_mg.at[2], temporalin_ref, 2 * width),
        (t_copies[1], t_nl, t_mg.at[1], temporalin_ref, width),
        (t_copies[0], t_nl, t_mg.at[0], temporalin_ref, 0),
        (s_early, s_c, s_att, spatialout_ref, 0),
        (s_copies[2], s_nl, s_mg.at[2], spatialin_ref, 2 * width),
        (s_copies[1], s_nl, s_mg.at[1], spatialin_ref, width),
        (s_copies[0], s_nl, s_mg.at[0], spatialin_ref, 0),
    ]
    pair_copies, row_copies = {}, {0: exit_rows}
    for slot in range(1, last_slot):
        needed, left, right, _, _ = work[slot]
        arrive(needed)
        pair_copies[slot] = partial(slot, left, right)
        if slot == 1:
            bot_pair_copy.wait_recv()
            bot_sum[...] = bot_send[...] + bot_pair[...]
            bot_recv[chip] = bot_sum[...]
            bot_copies = to_chips(lambda peer: bot_sum, bot_recv.at[chip], last_slot)
        else:
            row_copies[slot - 1] = pass_on(slot - 1, pair_copies[slot - 1])
    row_copies[last_slot - 1] = pass_on(last_slot - 1, pair_copies[last_slot - 1])

    arrive(bot_copies)
    bottle_total = bot_recv[0]
    for i in range(1, chips):
        bottle_total = bottle_total + bot_recv[i]
    bottle_delta_ref[...] = bottle_total.astype(BF16)
    for slot, (_, _, _, out, start) in enumerate(work):
        arrive(row_copies[slot])
        summed = row_recv[slot, 0].astype(F32)
        for i in range(1, chips):
            summed = summed + row_recv[slot, i].astype(F32)
        out[:, start : start + width] = (summed * grad_factor).astype(BF16)
    for copy in pending:
        copy.wait_send()


def hand_over(*refs):
    count = len(refs) // 2
    for source, target in zip(refs[:count], refs[count:]):
        target[...] = source[...]


def per_device(
    frames_in,
    bottleneck,
    spatial_entry,
    spatial_exit,
    temporal_entry,
    temporal_exit,
    output_grad,
    joined_grad,
):
    clip_count, frames_local, patches, model = frames_in.shape
    bottles = bottleneck.shape[1]
    frame_groups = lax.axis_size("frame")
    data_groups = lax.axis_size("dp")
    assert clip_count == 1 and frames_local == 1
    entry_width = spatial_entry.shape[1]
    exit_width = spatial_exit.shape[1]
    group = patches // frame_groups
    assert group & (group - 1) == 0 and frame_groups % 2 == 0
    assert entry_width == 3 * exit_width
    chips = frame_groups // 2
    rows = -(-(patches + bottles) // 16) * 16
    t_rows = patches
    block = model // data_groups
    owned = block // frame_groups
    grad_factor = 1.0 / math.sqrt(patches * data_groups * frame_groups)

    def gather_set(count):
        return [
            pltpu.VMEM((data_groups, count, block), BF16),
            pltpu.VMEM((data_groups, count, block), BF16),
            pltpu.VMEM((data_groups, count, exit_width), BF16),
            pltpu.VMEM((data_groups, count, block), BF16),
            pltpu.VMEM((data_groups, count, block), BF16),
            pltpu.VMEM((3, data_groups, count, exit_width), BF16),
        ]

    moved = pltpu.VMEM((frame_groups, group, model), BF16)
    vmem = pl.BlockSpec(memory_space=pltpu.VMEM)
    hbm = pl.BlockSpec(memory_space=pl.ANY)
    outs = pl.pallas_call(
        functools.partial(kernel, frame_groups, data_groups, grad_factor),
        out_shape=(
            jax.ShapeDtypeStruct((patches, model), BF16),
            jax.ShapeDtypeStruct((bottles, model), BF16),
            jax.ShapeDtypeStruct((owned, entry_width), BF16),
            jax.ShapeDtypeStruct((owned, exit_width), BF16),
            jax.ShapeDtypeStruct((owned, entry_width), BF16),
            jax.ShapeDtypeStruct((owned, exit_width), BF16),
        ),
        in_specs=[vmem] * 4 + [hbm] * 4,
        out_specs=[vmem] * 6,
        scratch_shapes=[
            pltpu.VMEM(spatial_entry.shape, BF16),
            pltpu.VMEM(spatial_exit.shape, BF16),
            pltpu.VMEM(temporal_entry.shape, BF16),
            pltpu.VMEM(temporal_exit.shape, BF16),
            pltpu.VMEM((rows, model), F32),
            pltpu.VMEM((rows, model), F32),
            pltpu.VMEM((rows, model), F32),
            pltpu.VMEM((t_rows, model), F32),
            moved,
            moved,
            moved,
            moved,
            moved,
            *[pltpu.VMEM((bottles, model), F32)] * 3,
            pltpu.VMEM((chips, bottles, model), F32),
            *gather_set(rows),
            *gather_set(t_rows),
            pltpu.VMEM((8, 2, chips, owned, exit_width), BF16),
            *[pltpu.VMEM((8, chips, owned, exit_width), BF16)] * 3,
            pltpu.SemaphoreType.DMA((4,)),
            pltpu.SemaphoreType.DMA((6, frame_groups)),
            pltpu.SemaphoreType.DMA((6, frame_groups)),
            pltpu.SemaphoreType.DMA((12, data_groups)),
            pltpu.SemaphoreType.DMA((12, data_groups)),
            pltpu.SemaphoreType.DMA((2, 9)),
            pltpu.SemaphoreType.DMA((9, chips)),
            pltpu.SemaphoreType.DMA((9, chips)),
        ],
        compiler_params=pltpu.CompilerParams(
            collective_id=0, has_side_effects=True, vmem_limit_bytes=61 * 1024 * 1024
        ),
    )(
        frames_in.reshape(patches, model),
        bottleneck.reshape(bottles, model),
        output_grad.reshape(frame_groups, group, model),
        joined_grad.reshape(bottles, model),
        spatial_entry,
        spatial_exit,
        temporal_entry,
        temporal_exit,
    )
    outs = pl.pallas_call(
        hand_over,
        out_shape=[jax.ShapeDtypeStruct(out.shape, out.dtype) for out in outs],
        in_specs=[vmem] * len(outs),
        out_specs=[vmem] * len(outs),
        compiler_params=pltpu.CompilerParams(vmem_limit_bytes=61 * 1024 * 1024),
    )(*outs)
    return (outs[0].reshape(frames_in.shape), outs[1].reshape(bottleneck.shape), *outs[2:])


def solution(mesh):
    return jax.shard_map(
        per_device,
        mesh=mesh,
        in_specs=(
            P("dp", "frame", None, None),
            P("dp", None, None),
            P(),
            P(),
            P(),
            P(),
            P("dp", "frame", None, None),
            P("dp", None, None),
        ),
        out_specs=(
            P("dp", "frame", None, None),
            P("dp", None, None),
            P(("dp", "frame"), None),
            P(("dp", "frame"), None),
            P(("dp", "frame"), None),
            P(("dp", "frame"), None),
        ),
        check_vma=False,
    )
```
